8 devices in a mesh: seqs: 1 (over z), rows: 2 (over y), states: 4 (over x, core).
Axes of the slice: x: 2, y: 2, z: 1, core: 2. Of those that a mesh axis runs over, the one named last changes fastest.
Arguments:
- trans_mat: bfloat16 [4096, 2, 2048], P('rows', None, 'states')
- emit_mat: bfloat16 [4096, 50257], P(('rows', 'states'))
- init_dist: float32 [4096], P(('rows', 'states'))
- tokens: int32 [64, 4], P('seqs')
- lengths: int32 [64], P('seqs')
Outputs:
- output 1: float32 [64], P('seqs')
- output 2: float32 [64, 4096], P('seqs', ('rows', 'states'))
All inputs are finite; a program needn't handle non-finite values.
Results may differ from the reference program's by a relative error of at most 0.001.
Values are sent between devices in bfloat16 or wider.
A program may use at most 1 GiB of HBM per device.

```python
import jax
import jax.numpy as jnp
from jax import lax
import functools

STATES = 4096
VOCAB = 50257
BATCH = 64
STEPS = 4
ROW_SPLIT = 2
DRAW_ROWS = 256


def draw_rows(key, n_cols, sharpness):
    logits = sharpness * jax.random.normal(key, (DRAW_ROWS, n_cols), jnp.float32)
    return jax.nn.softmax(logits, axis=1).astype(jnp.bfloat16)


def draw_sequences(key):
    key_tok, key_len, key_long, key_short = jax.random.split(key, 4)
    tokens = jax.random.randint(key_tok, (BATCH, STEPS), 0, VOCAB, dtype=jnp.int32)
    lengths = jax.random.randint(key_len, (BATCH,), 1, STEPS + 1, dtype=jnp.int32)
    long_row = jax.random.randint(key_long, (), 0, BATCH, dtype=jnp.int32)
    short_row = (long_row + 1 + jax.random.randint(key_short, (), 0, BATCH - 1, dtype=jnp.int32)) % BATCH
    lengths = lengths.at[long_row].set(STEPS).at[short_row].set(1)
    return tokens, lengths


def setup_inputs(seed: int = 0, part: int = 0) -> dict:
    base_key = jax.random.key(seed)
    key_trans, key_emit, key_init, key_seq = jax.random.split(base_key, 4)
    n_blocks = STATES // DRAW_ROWS
    trans_rows = lax.map(functools.partial(draw_rows, n_cols=STATES, sharpness=2.5), jax.random.split(key_trans, n_blocks))
    emit_rows = lax.map(functools.partial(draw_rows, n_cols=VOCAB, sharpness=2.0), jax.random.split(key_emit, n_blocks))
    init_dist = jax.nn.softmax(1.5 * jax.random.normal(key_init, (STATES,), jnp.float32))
    tokens, lengths = draw_sequences(jax.random.fold_in(key_seq, part))
    return {'trans_mat': trans_rows.reshape(STATES, ROW_SPLIT, STATES // ROW_SPLIT), 'emit_mat': emit_rows.reshape(STATES, VOCAB), 'init_dist': init_dist, 'tokens': tokens, 'lengths': lengths}


def emission(emit_mat, step_tok):
    return jnp.take(emit_mat, step_tok, axis=1).T.astype(jnp.float32)


def reference(trans_mat, emit_mat, init_dist, tokens, lengths):
    trans_full = trans_mat.reshape(STATES, STATES)
    first_raw = init_dist[None, :] * emission(emit_mat, tokens[:, 0])
    norm_c = jnp.sum(first_raw, axis=1)
    alpha_init = first_raw / norm_c[:, None]
    loglik_init = jnp.log(norm_c)

    def one_step(state_in, inputs):
        alpha_cur, loglik = state_in
        step_tok, t_index = inputs
        mix_sum = jnp.dot(alpha_cur.astype(jnp.bfloat16), trans_full, preferred_element_type=jnp.float32)
        raw_next = mix_sum * emission(emit_mat, step_tok)
        norm_step = jnp.sum(raw_next, axis=1)
        active = t_index < lengths
        alpha_cur = jnp.where(active[:, None], raw_next / norm_step[:, None], alpha_cur)
        loglik = loglik + jnp.where(active, jnp.log(norm_step), 0.0)
        return (alpha_cur, loglik), None

    scan_out = lax.scan(one_step, (alpha_init, loglik_init), (tokens[:, 1:].T, jnp.arange(1, STEPS)))
    alpha_last, loglik = scan_out[0]
    return loglik, alpha_last
```

```python
import functools

import jax
import jax.numpy as jnp
from jax import lax
from jax.experimental import pallas as pl
from jax.experimental.pallas import tpu as pltpu
from jax.sharding import PartitionSpec as P

MESH = pl.DeviceIdType.MESH
F32, BF16 = jnp.float32, jnp.bfloat16
LANES, SUBL = 128, 8


def fold_rows(col, groups):
    lane = lax.broadcasted_iota(jnp.int32, (SUBL, LANES), 1)
    out = jnp.zeros((SUBL, LANES), F32)
    for g in range(groups):
        out = jnp.where(lane == g, col[g * SUBL:(g + 1) * SUBL], out)
    return out


def spread_rows(folded, groups):
    return jnp.concatenate([folded[:, g:g + 1] for g in range(groups)], axis=0)


def interleave(block, out_ref):
    rows, cols = block.shape
    x = block.astype(F32)
    lane = lax.broadcasted_iota(jnp.int32, (rows, LANES), 1)
    for j in range(cols // LANES):
        xj = x[:, j * LANES:(j + 1) * LANES]
        for h in range(2):
            g = jnp.take_along_axis(xj, lane // 2 + h * (LANES // 2), axis=1)
            c0 = (2 * j + h) * LANES
            out_ref[0:rows, c0:c0 + LANES] = jnp.where(lane % 2 == 0, g, 0.0).astype(BF16)
            out_ref[rows:2 * rows, c0:c0 + LANES] = jnp.where(lane % 2 == 1, g, 0.0).astype(BF16)


def kernel(n_steps, len_ref, emis_ref, init_ref, trans_hbm, ll_ref, alpha_ref,
           trans, emis_row, init_row, emis_col, c_out, c_in, part, u_in, a_out, a_in, left,
           load_sem, s_sem, r_sem):
    batch, q = alpha_ref.shape
    groups = batch // SUBL
    z = lax.axis_index('seqs')
    i = lax.axis_index('rows')
    s = lax.axis_index('states')
    x, c = s // 2, s % 2

    def peer(d):
        dy, dx, dc = d // 4, (d // 2) % 2, d % 2
        return (z, 1 - i if dy else i, 2 * (1 - x if dx else x) + (1 - c if dc else c))

    load = pltpu.make_async_copy(trans_hbm.reshape(trans.shape), trans, load_sem)
    load.start()

    barrier = pltpu.get_barrier_semaphore()
    for d in range(1, 8):
        pl.semaphore_signal(barrier, inc=1, device_id=peer(d), device_id_type=MESH)
    pl.semaphore_wait(barrier, 7)

    sent = []

    def send(src, dst, d):
        k = len(sent)
        cp = pltpu.make_async_remote_copy(src_ref=src, dst_ref=dst, send_sem=s_sem.at[k], recv_sem=r_sem.at[k], device_id=peer(d), device_id_type=MESH)
        cp.start()
        sent.append(cp)
        return cp

    def send_c(t, partial):
        c_out[t] = fold_rows(jnp.sum(partial, axis=1, keepdims=True), groups)
        return [send(c_out.at[t], c_in.at[t, d - 1], d) for d in range(1, 8)]

    def recv_c(t, copies):
        for cp in copies:
            cp.wait_recv()
        total = c_out[t]
        for d in range(1, 8):
            total = total + c_in[t, d - 1]
        return total

    def lane_sum(v):
        out = v[:, 0:LANES]
        for j in range(1, q // LANES):
            out = out + v[:, j * LANES:(j + 1) * LANES]
        return out

    copies_e = [send(emis_ref.at[0], emis_row.at[d - 1], d) for d in (1, 2, 3)]
    copies_p = [send(init_ref, init_row.at[d - 1], d) for d in (1, 2, 3)]
    raw = init_ref[...] * emis_ref[0].astype(F32)
    copies_c = send_c(0, lane_sum(raw))
    copies_ep = [send(emis_ref.at[t], emis_col.at[t - 1], 4) for t in range(1, n_steps)]

    sub = lax.broadcasted_iota(jnp.int32, (SUBL, LANES), 0)
    lane = lax.broadcasted_iota(jnp.int32, (SUBL, LANES), 1)
    lens = jnp.zeros((SUBL, LANES), jnp.int32)
    for b in range(batch):
        lens = jnp.where((sub == b % SUBL) & (lane == b // SUBL), len_ref[b], lens)

    c_tot = recv_c(0, copies_c)
    ll = jnp.log(c_tot)
    c_col = spread_rows(c_tot, groups)
    alpha = raw / c_col
    alpha_ref[...] = alpha
    interleave(alpha.astype(BF16), left.at[0])
    for d in (1, 2, 3):
        copies_e[d - 1].wait_recv()
        copies_p[d - 1].wait_recv()
        blk = (init_row[d - 1] * emis_row[d - 1].astype(F32)) / c_col
        interleave(blk.astype(BF16), left.at[d])
    load.wait()

    for t in range(1, n_steps):
        acc = None
        for d in range(4):
            if t > 1 and d > 0:
                copies_a[d - 1].wait_recv()
                interleave(a_in[t - 2, d - 1], left.at[d])
            sp = peer(d)[2]
            rows = pl.ds(pl.multiple_of(sp * 2 * q, 2 * q), 2 * q)
            prod = jnp.dot(left[d], trans[rows, :], preferred_element_type=F32)
            acc = prod if acc is None else acc + prod
        part[t - 1] = acc
        mine = pl.ds(pl.multiple_of(i * batch, batch), batch)
        other = pl.ds(pl.multiple_of((1 - i) * batch, batch), batch)
        copy_u = send(part.at[t - 1, other], u_in.at[t - 1], 4)
        emis_t = emis_ref[t].astype(F32)
        copies_ep[t - 1].wait_recv()
        own = part[t - 1, mine]
        w = own * emis_t + part[t - 1, other] * emis_col[t - 1].astype(F32)
        copies_c = send_c(t, lane_sum(w))
        copy_u.wait_recv()
        raw = (own + u_in[t - 1]) * emis_t
        c_tot = recv_c(t, copies_c)
        active = lens > t
        ll = ll + jnp.where(active, jnp.log(c_tot), 0.0)
        c_col = spread_rows(c_tot, groups)
        act_col = spread_rows(active.astype(F32), groups)
        alpha = jnp.where(act_col > 0.5, raw / c_col, alpha_ref[...])
        alpha_ref[...] = alpha
        if t < n_steps - 1:
            a_out[t - 1] = alpha.astype(BF16)
            copies_a = [send(a_out.at[t - 1], a_in.at[t - 1, d - 1], d) for d in (1, 2, 3)]
            interleave(alpha.astype(BF16), left.at[0])

    ll = jnp.where(lane < groups, ll, 0.0)
    wide = jnp.take_along_axis(ll, lane // SUBL, axis=1)
    ll_ref[...] = jnp.sum(jnp.where(lane % SUBL == sub, wide, 0.0), axis=0, keepdims=True)[:, :batch]
    for cp in sent:
        cp.wait_send()


def solution(mesh):
    vec_axes = ('rows', 'states')

    def local_forward(trans_blk, emit_blk, init_blk, tokens, lengths):
        batch, n_steps = tokens.shape
        src, two, q = trans_blk.shape
        toks = tokens.T.reshape(-1)
        emis = jnp.take(emit_blk.T, toks, axis=0, mode='clip').reshape(n_steps, batch, q)
        n_copies = 3 + 3 + 7 * n_steps + (n_steps - 1) * 2 + 3 * (n_steps - 2)
        vmem = pl.BlockSpec(memory_space=pltpu.VMEM)
        ll, alpha = pl.pallas_call(
            functools.partial(kernel, n_steps),
            out_shape=(jax.ShapeDtypeStruct((1, batch), F32), jax.ShapeDtypeStruct((batch, q), F32)),
            in_specs=[pl.BlockSpec(memory_space=pltpu.SMEM), vmem, vmem, pl.BlockSpec(memory_space=pl.ANY)],
            out_specs=(vmem, vmem),
            scratch_shapes=[
                pltpu.VMEM((2 * src, q), BF16),
                pltpu.VMEM((3, batch, q), BF16),
                pltpu.VMEM((3, 1, q), F32),
                pltpu.VMEM((n_steps - 1, batch, q), BF16),
                pltpu.VMEM((n_steps, SUBL, LANES), F32),
                pltpu.VMEM((n_steps, 7, SUBL, LANES), F32),
                pltpu.VMEM((n_steps - 1, 2 * batch, q), F32),
                pltpu.VMEM((n_steps - 1, batch, q), F32),
                pltpu.VMEM((n_steps - 2, batch, q), BF16),
                pltpu.VMEM((n_steps - 2, 3, batch, q), BF16),
                pltpu.VMEM((4, 2 * batch, 2 * q), BF16),
                pltpu.SemaphoreType.DMA,
                pltpu.SemaphoreType.DMA((n_copies,)),
                pltpu.SemaphoreType.DMA((n_copies,)),
            ],
            compiler_params=pltpu.CompilerParams(collective_id=0, has_side_effects=True),
        )(lengths, emis, init_blk.reshape(1, q), trans_blk)
        return ll.reshape(batch), alpha

    return jax.shard_map(local_forward, mesh=mesh, in_specs=(P('rows', None, 'states'), P(vec_axes, None), P(vec_axes), P('seqs', None), P('seqs')), out_specs=(P('seqs'), P('seqs', vec_axes)), check_vma=False)
```
